32 devices in a mesh: seq: 8 (over z, x), head: 4 (over y, core).
Axes of the slice: x: 2, y: 2, z: 4, core: 2. Of those that a mesh axis runs over, the one named last changes fastest.
Arguments:
- queries: bfloat16 [8192, 2048], P('seq', 'head'), may hold values from -200 to 200
- keys: bfloat16 [8192, 2048], P('seq', 'head'), may hold values from -6 to 6
- values: bfloat16 [8192, 2048], P('seq', 'head'), may hold values from -12 to 12
- gate_bias: float32 [16], P('head'), may hold values from -2 to 2
- out_weight: bfloat16 [2048, 4096], P(None, 'head'), may hold values from -0.125 to 0.125
Outputs:
- layer_out: bfloat16 [8192, 4096], P('seq', 'head')
The draws below stay inside these ranges and needn't reach their ends.
All inputs are finite; a program needn't handle non-finite values.
Results may differ from the reference program's by a relative error of at most 0.007.
Values may be sent and summed in bfloat16 or wider, within the bound.
A program may use at most 128 MiB of HBM per device.

```python
import jax
import jax.numpy as jnp
from jax import lax

D = 4096
HEADS = 16
DH = 128
SEG = 256
TOKENS = 8192


def sign_field(key, salt, shape):
    flips = jax.random.bernoulli(jax.random.fold_in(key, salt), 0.5, shape)
    return jnp.where(flips, 1.0, -1.0).astype(jnp.float32)


def column_pattern(key):
    per_segment = sign_field(key, 21, (TOKENS // SEG, HEADS * DH))
    return jnp.repeat(per_segment, SEG, axis=0)


def key_signs(key):
    rates = jax.random.uniform(jax.random.fold_in(key, 24), (TOKENS // SEG, HEADS), jnp.float32, 0.2, 0.8)
    coins = jax.random.uniform(jax.random.fold_in(key, 22), (TOKENS, HEADS), jnp.float32)
    signs = jnp.where(coins < jnp.repeat(rates, SEG, axis=0), 1.0, -1.0).astype(jnp.float32)
    return jnp.repeat(signs, DH, axis=1)


def query_signs(key):
    return jnp.repeat(sign_field(key, 23, (TOKENS, HEADS)), DH, axis=1)


def position_shift():
    positions = jnp.arange(TOKENS).astype(jnp.float32)
    return -1.5 + 3.0 * (positions + 0.5) / TOKENS


def key_table(key):
    noise = jax.random.normal(jax.random.fold_in(key, 11), (TOKENS, HEADS * DH), jnp.float32)
    table = noise + 2.0 * key_signs(key) * column_pattern(key) + position_shift()[:, None]
    return jnp.clip(table, -6.0, 6.0)


def draw_keys(key, part):
    return key_table(key).astype(jnp.bfloat16)


def draw_queries(key, part):
    base_draw = jax.random.normal(jax.random.fold_in(key, 12), (TOKENS, HEADS * DH), jnp.float32)
    base_draw = base_draw + 0.75 * query_signs(key) * column_pattern(key)
    return jnp.clip(base_draw, -200.0, 200.0).astype(jnp.bfloat16)


def draw_values(key, part):
    noise = jax.random.normal(jax.random.fold_in(key, 13), (TOKENS, HEADS * DH), jnp.float32)
    column_off = jax.random.normal(jax.random.fold_in(key, 14), (HEADS * DH,), jnp.float32)
    segment_off = jax.random.normal(jax.random.fold_in(key, 15), (TOKENS // SEG, HEADS * DH), jnp.float32)
    linked = jax.random.normal(jax.random.fold_in(key, 16), (TOKENS // SEG, HEADS * DH), jnp.float32)
    table = noise + column_off[None, :] + jnp.repeat(segment_off, SEG, axis=0)
    table = table + 1.5 * key_signs(key) * jnp.repeat(linked, SEG, axis=0)
    return jnp.clip(table, -12.0, 12.0).astype(jnp.bfloat16)


def shard_levels(stream_key, shape, split, least, top_value):
    gain = 1.0
    for dim, parts in split:
        heights = jax.random.uniform(jax.random.fold_in(jax.random.fold_in(stream_key, 6), dim), (parts,), jnp.float32, least / len(split), top_value / len(split))
        gain = gain * jnp.repeat(jnp.exp(heights), shape[dim] // parts).reshape((-1,) + (1,) * (len(shape) - 1 - dim))
    return gain


def scatter_about(own_key, dims, spread, bound, pieces=(), held_as=jnp.bfloat16):
    array = spread * jax.random.normal(own_key, dims, jnp.float32)
    if pieces:
        array = array * shard_levels(own_key, dims, pieces, -0.22, 0.18)
    return jnp.clip(array, -bound, bound).astype(held_as)


def setup_inputs(seed: int = 0) -> dict:
    key_list = jax.random.split(jax.random.key(seed), 6)
    return {
        "queries": draw_queries(jax.random.fold_in(key_list[5], 71), 0),
        "keys": draw_keys(jax.random.fold_in(key_list[5], 71), 0),
        "values": draw_values(jax.random.fold_in(key_list[5], 71), 0),
        "gate_bias": jnp.clip(jax.random.uniform(key_list[3], (HEADS,), jnp.float32, -2.0, 2.0) * shard_levels(key_list[3], (HEADS,), ((0, 4),), -0.4, 0.0), -2.0, 2.0),
        "out_weight": scatter_about(key_list[4], (HEADS * DH, D), (HEADS * DH) ** -0.5, 0.125, ((1, 4),)),
    }


def reference(queries, keys, values, gate_bias, out_weight):
    seg_count = TOKENS // SEG
    blk_shape = (seg_count, SEG, HEADS, DH)
    query_blk = queries.reshape(blk_shape)
    key_blk = keys.reshape(blk_shape)
    value_blk = values.reshape(blk_shape)
    gate_open = jax.nn.sigmoid(gate_bias.astype(jnp.float32))
    positions = jnp.arange(SEG)
    causal = positions[:, None] >= positions[None, :]
    score_scale = 1.0 / (DH ** 0.5)
    high = lax.Precision.HIGHEST

    def segment(state_pair, inputs_seg):
        memory, normalizer = state_pair
        query_seg, key_seg, value_seg = inputs_seg
        query_flt = query_seg.astype(jnp.float32)
        key_flt = key_seg.astype(jnp.float32)
        value_flt = value_seg.astype(jnp.float32)
        query_map = jax.nn.elu(query_flt) + 1.0
        key_map = (jax.nn.elu(key_flt) + 1.0).astype(jnp.bfloat16).astype(jnp.float32)
        recall = jnp.einsum('thd,hde->the', query_map, memory, precision=high)
        denominator = jnp.einsum('thd,hd->th', query_map, normalizer, precision=high) + 1.0
        recall = recall / denominator[:, :, None]
        scores = jnp.einsum('qhd,khd->hqk', query_flt, key_flt, precision=high) * score_scale
        scores = jnp.where(causal[None], scores, jnp.float32(-1e30))
        weights = jax.nn.softmax(scores, axis=-1).astype(jnp.bfloat16).astype(jnp.float32)
        local_out = jnp.einsum('hqk,khd->qhd', weights, value_flt, precision=high)
        mixed = gate_open[None, :, None] * recall + (1.0 - gate_open)[None, :, None] * local_out
        context = mixed.astype(jnp.bfloat16).reshape(SEG, HEADS * DH)
        projected = jnp.dot(context, out_weight, preferred_element_type=jnp.float32).astype(jnp.bfloat16)
        memory = memory + jnp.einsum('thd,the->hde', key_map, value_flt, precision=high)
        normalizer = normalizer + jnp.sum(key_map, axis=0)
        return (memory, normalizer), projected

    start_state = (jnp.zeros((HEADS, DH, DH), jnp.float32), jnp.zeros((HEADS, DH), jnp.float32))
    ignored, outputs = lax.scan(segment, start_state, (query_blk, key_blk, value_blk))
    return outputs.reshape(TOKENS, D)
```

```python
import functools

import jax
import jax.numpy as jnp
from jax import lax
from jax.experimental import pallas as pl
from jax.experimental.pallas import tpu as pltpu
from jax.sharding import PartitionSpec as P

DH = 128
SEG = 256
MEM = DH + 8
PAIR = 2 * DH
MESH = pl.DeviceIdType.MESH
F32 = jnp.float32
BF16 = jnp.bfloat16
NT = (((1,), (1,)), ((), ()))
TN = (((0,), (0,)), ((), ()))


def elu1(x):
    return jnp.where(x > 0.0, x + 1.0, jnp.exp(jnp.minimum(x, 0.0)))


def split(x):
    top = x.astype(BF16)
    return top, (x - top.astype(F32)).astype(BF16)


def kernel(
    ns, nh, q_ref, k_ref, v_ref, gate_ref, w_hbm, out_ref,
    w_ref, local, inner, total, from_pair, from_prev, to_next, prior, ctx, acc,
    w_sem, x_send, x_recv, z_send, z_recv, c_send, c_recv, f_send,
):
    rows, cols = q_ref.shape
    segs, heads = rows // SEG, cols // DH
    pairs = heads // 2
    blocks = segs * heads
    me_s, me_h = lax.axis_index("seq"), lax.axis_index("head")
    z, odd = me_s // 2, lax.rem(me_s, 2)
    zs = ns // 2
    pair_s = me_s + 1 - 2 * odd
    up, down = lax.rem(me_s + 2, ns), lax.rem(me_s + ns - 2, ns)
    group, core = me_h // 2, lax.rem(me_h, 2)
    pair_h = me_h + 1 - 2 * core
    groups = nh // 2

    weight_copy = pltpu.make_async_copy(w_hbm, w_ref, w_sem)
    weight_copy.start()

    barrier = pltpu.get_barrier_semaphore()
    seq_peers = [pair_s, up, down]
    for s in seq_peers:
        pl.semaphore_signal(barrier, inc=1, device_id=(s, me_h), device_id_type=MESH)
    far = [lax.rem(group + d, groups) * 2 + core for d in range(1, groups)]
    for h in [pair_h] + far:
        pl.semaphore_signal(barrier, inc=1, device_id=(me_s, h), device_id_type=MESH)

    def x_copy(h):
        return pltpu.make_async_remote_copy(
            src_ref=total.at[h], dst_ref=from_pair.at[h],
            send_sem=x_send.at[h], recv_sem=x_recv.at[h],
            device_id=(pair_s, me_h), device_id_type=MESH,
        )

    def z_copy(h):
        return pltpu.make_async_remote_copy(
            src_ref=to_next.at[h], dst_ref=from_prev.at[h],
            send_sem=z_send.at[h], recv_sem=z_recv.at[h],
            device_id=(up, me_h), device_id_type=MESH,
        )

    def ctx_copy(source, target, j, s, send):
        part = ctx.at[source * pairs + j, pl.ds(pl.multiple_of(s * SEG, SEG), SEG)]
        return pltpu.make_async_remote_copy(
            src_ref=part, dst_ref=part,
            send_sem=send, recv_sem=c_recv.at[source, j, s],
            device_id=(me_s, target), device_id_type=MESH,
        )

    for h in range(heads):
        span = pl.ds(h * DH, DH)
        run = jnp.zeros((MEM, DH), F32)
        for s in range(segs):
            inner[h, s] = run
            part = pl.ds(s * SEG, SEG)
            key_map = elu1(k_ref[part, span].astype(F32)).astype(BF16)
            delta = lax.dot_general(v_ref[part, span], key_map, TN, preferred_element_type=F32)
            norm = jnp.sum(key_map.astype(F32), axis=0, keepdims=True)
            run = run + jnp.concatenate([delta, jnp.broadcast_to(norm, (8, DH))], axis=0)
        total[h] = run
        if h == 0:
            pl.semaphore_wait(barrier, 3 + 1 + len(far))
        x_copy(h).start()

    @pl.when(z == 0)
    def _():
        from_prev[...] = jnp.zeros_like(from_prev)

    def chain(h):
        x_copy(h).wait_recv()

        @pl.when(z > 0)
        def _():
            z_copy(h).wait_recv()

        before = from_prev[h]
        other = from_pair[h]

        @pl.when(z < zs - 1)
        def _():
            to_next[h] = before + (total[h] + other)
            z_copy(h).start()

        prior[h] = before + jnp.where(odd == 1, other, 0.0)

    row_id = lax.broadcasted_iota(jnp.int32, (SEG, SEG), 0)
    col_id = lax.broadcasted_iota(jnp.int32, (SEG, SEG), 1)
    ones = jnp.ones((SEG, DH), BF16)
    first, hop = 3, 5

    @pl.loop(0, blocks)
    def _(b):
        for c in range(heads):
            @pl.when(b == first + 2 * c + hop * z)
            def _():
                chain(c)
        h, s = b // segs, lax.rem(b, segs)
        span = pl.ds(pl.multiple_of(h * DH, DH), DH)
        part = pl.ds(pl.multiple_of(s * SEG, SEG), SEG)
        scores = lax.dot_general(q_ref[part, span], k_ref[part, span], NT, preferred_element_type=F32)
        scores = jnp.where(row_id >= col_id, scores * (1.0 / DH**0.5), -1e30)
        weights = jnp.exp(scores - jnp.max(scores, axis=1, keepdims=True)).astype(BF16)
        both = jnp.dot(
            weights, jnp.concatenate([v_ref[part, span], ones], axis=1), preferred_element_type=F32
        )
        local[part, span] = both[:, :DH] / both[:, DH:]

    for c in range(heads):
        @pl.when(first + 2 * c + hop * z >= blocks)
        def _():
            chain(c)

    for j in range(pairs):
        gates = [
            1.0 / (1.0 + jnp.exp(-jnp.full((1, DH), gate_ref[2 * j + i], F32))) for i in range(2)
        ]

        @pl.loop(0, segs)
        def _(s):
            part = pl.ds(pl.multiple_of(s * SEG, SEG), SEG)
            mixed = []
            for i in range(2):
                h = 2 * j + i
                span = pl.ds(h * DH, DH)
                mem = prior[h] + inner[h, s]
                mem = jnp.concatenate(
                    [mem[:DH], jnp.broadcast_to(mem[DH : DH + 1], (DH, DH))], axis=0
                )
                m_top, m_low = split(mem)
                q_top, q_low = split(elu1(q_ref[part, span].astype(F32)))
                recall = lax.dot_general(
                    jnp.concatenate([q_top, q_low], axis=1),
                    jnp.concatenate([m_top, m_top], axis=1),
                    NT, preferred_element_type=F32,
                ) + lax.dot_general(q_top, m_low, NT, preferred_element_type=F32)
                recall = recall[:, :DH] / (recall[:, DH:] + 1.0)
                mixed.append(gates[i] * recall + (1.0 - gates[i]) * local[part, span])
            ctx[me_h * pairs + j, part] = jnp.concatenate(mixed, axis=1).astype(BF16)
            for t in far + [pair_h]:
                ctx_copy(me_h, t, j, s, c_send.at[t, j, s]).start()

    weight_copy.wait()

    def product(source, j, part):
        slot = source * pairs + j
        return jnp.dot(
            ctx[slot, part],
            w_ref[pl.ds(pl.multiple_of(slot * PAIR, PAIR), PAIR), :],
            preferred_element_type=F32,
        )

    @pl.loop(0, segs)
    def _(s):
        part = pl.ds(pl.multiple_of(s * SEG, SEG), SEG)
        for j in range(pairs):
            ctx_copy(pair_h, pair_h, j, s, c_send.at[pair_h, j, s]).wait_recv()
        sums = product(me_h, 0, part)
        for j in range(1, pairs):
            sums = sums + product(me_h, j, part)
        for j in range(pairs):
            sums = sums + product(pair_h, j, part)
        acc[part, :] = sums

    for j in range(pairs):
        for f in far:
            twin = (f // 2) * 2 + 1 - core

            @pl.loop(0, segs)
            def _(s):
                part = pl.ds(pl.multiple_of(s * SEG, SEG), SEG)
                ctx_copy(f, pair_h, j, s, c_send.at[f, j, s]).wait_recv()
                ctx_copy(f, pair_h, j, s, f_send.at[f, j, s]).start()
                sums = acc[part, :] + product(f, j, part)
                ctx_copy(twin, pair_h, j, s, c_send.at[f, j, s]).wait_recv()
                acc[part, :] = sums + product(twin, j, part)

    out_ref[...] = acc[...].astype(BF16)

    for h in range(heads):
        x_copy(h).wait_send()

        @pl.when(z < zs - 1)
        def _():
            z_copy(h).wait_send()

    for j in range(pairs):
        @pl.loop(0, segs)
        def _(s):
            for t in far + [pair_h]:
                ctx_copy(me_h, t, j, s, c_send.at[t, j, s]).wait_send()
            for f in far:
                ctx_copy(f, pair_h, j, s, f_send.at[f, j, s]).wait_send()


def body(ns, nh, queries, keys, values, gate_bias, out_weight):
    rows, cols = queries.shape
    depth, outs = out_weight.shape
    segs, heads = rows // SEG, cols // DH
    pairs = heads // 2
    vmem = pl.BlockSpec(memory_space=pltpu.VMEM)
    dma = pltpu.SemaphoreType.DMA
    mem = pltpu.VMEM((heads, MEM, DH), F32)
    return pl.pallas_call(
        functools.partial(kernel, ns, nh),
        out_shape=jax.ShapeDtypeStruct((rows, outs), BF16),
        in_specs=[vmem, vmem, vmem, pl.BlockSpec(memory_space=pltpu.SMEM),
                  pl.BlockSpec(memory_space=pl.ANY)],
        out_specs=vmem,
        scratch_shapes=[
            pltpu.VMEM((depth, outs), BF16),
            pltpu.VMEM((rows, cols), F32),
            pltpu.VMEM((heads, segs, MEM, DH), F32),
            mem, mem, mem, mem, mem,
            pltpu.VMEM((nh * pairs, rows, PAIR), BF16),
            pltpu.VMEM((rows, outs), F32),
            dma, dma((heads,)), dma((heads,)), dma((heads,)), dma((heads,)),
            dma((nh, pairs, segs)), dma((nh, pairs, segs)), dma((nh, pairs, segs)),
        ],
        compiler_params=pltpu.CompilerParams(
            collective_id=0, has_side_effects=True, vmem_limit_bytes=60 * 1024 * 1024
        ),
        name="infini_layer",
    )(queries, keys, values, gate_bias, out_weight)


def solution(mesh):
    sizes = dict(mesh.shape)
    return jax.shard_map(
        functools.partial(body, sizes["seq"], sizes["head"]),
        mesh=mesh,
        in_specs=(P("seq", "head"), P("seq", "head"), P("seq", "head"), P("head"), P(None, "head")),
        out_specs=P("seq", "head"),
        check_vma=False,
    )
```
